32 devices in a mesh: slab: 8 (over z, y), pencil: 4 (over x, core).
Axes of the slice: x: 2, y: 2, z: 4, core: 2. Of those that a mesh axis runs over, the one named last changes fastest.
Arguments:
- density_history: float32 [7, 64, 320, 320], P(None, 'slab', 'pencil'), may hold values from -6 to 6
- residual_history: float32 [7, 64, 320, 320], P(None, 'slab', 'pencil'), as said below
- occupancy_history: float32 [7, 768, 324], P(None, ('slab', 'pencil')), may hold values from -6 to 6
- occupancy_residual: float32 [7, 768, 324], P(None, ('slab', 'pencil')), may hold values from -6 to 6
- species: int32 [768], P(('slab', 'pencil')), may hold values from 0 to 3
- slot_count: int32 [32], P(('slab', 'pencil')), may hold values from 12 to 24, as said below
Outputs:
- new_density: float32 [64, 320, 320], P('slab', 'pencil')
- new_occupancy: float32 [768, 324], P(('slab', 'pencil'))
The draws below stay inside these ranges and needn't reach their ends.
Inputs may be any that keep to these rules, and one draw needn't show every extreme that they name: `residual_history`: residual fields of the 7 previous steps. Device d of slab+pencil (slab slowest) holds slots d * 24 to (d + 1) * 24 - 1, of which the first slot_count[d] hold atoms; some device is full in every draw.
All inputs are finite; a program needn't handle non-finite values.
Results may differ from the reference program's by a relative error of at most 0.00017.
Values sent between devices are 32-bit elements; how exact they have to be, the bound alone decides.
A program may use at most 128 MiB of HBM per device.

```python
import math
import jax
import jax.numpy as jnp
from jax import lax

HISTORY = 7
NX = 320
NY = 320
NZ = 64
ORBITALS = 18
SLOT_DEV = 24
SLOTS = 768


def smooth_lines(key, leading, length):
    keys = jax.random.split(key, 2)
    amplitude = 0.5 * jax.random.normal(keys[0], leading + (4,), jnp.float32)
    phase = jax.random.uniform(keys[1], leading + (4,), jnp.float32, 0.0, 2.0 * math.pi)
    position = jnp.arange(length, dtype=jnp.float32)
    wavenumber = jnp.arange(1, 5, dtype=jnp.float32)
    angle = 2.0 * math.pi * wavenumber[:, None] * position[None, :] / length
    return jnp.sum(amplitude[..., None] * jnp.cos(angle + phase[..., None]), axis=-2)


def region_scale(key, length, upper):
    return jnp.exp(jax.random.uniform(key, (length,), jnp.float32, 0.0, math.log(upper)))


def draw_residual_history(key, part):
    keys = jax.random.split(key, 11)
    shared = 0.6
    spread = 4.0
    upper = 3.0
    common_noise = jax.random.normal(keys[0], (NZ, NY, NX), jnp.float32)
    own_noise = jax.random.normal(keys[1], (HISTORY, NZ, NY, NX), jnp.float32)
    region = region_scale(keys[2], NZ, upper)[:, None, None] * region_scale(keys[3], NY, upper)[None, :, None] * region_scale(keys[4], NX, upper)[None, None, :]
    common_smooth = smooth_lines(keys[5], (), NZ)[:, None, None] + smooth_lines(keys[6], (), NY)[None, :, None] + smooth_lines(keys[7], (), NX)[None, None, :]
    own_smooth = smooth_lines(keys[8], (HISTORY,), NZ)[:, :, None, None] + smooth_lines(keys[9], (HISTORY,), NY)[:, None, :, None] + smooth_lines(keys[10], (HISTORY,), NX)[:, None, None, :]
    common = common_noise * region + common_smooth
    own = own_noise * region[None] + own_smooth
    step_index = jnp.arange(HISTORY, dtype=jnp.float32)
    history_scale = jnp.exp(math.log(spread) * (1.0 - step_index / max(HISTORY - 1, 1)))
    value = history_scale[:, None, None, None] * (shared * common[None] + math.sqrt(1.0 - shared * shared) * own)
    return value.astype(jnp.float32)


def draw_slot_count(key, part):
    keys = jax.random.split(key, 2)
    devices_total = SLOTS // SLOT_DEV
    counts = jax.random.randint(keys[0], (devices_total,), max(1, SLOT_DEV // 2), SLOT_DEV + 1)
    filled = jax.random.randint(keys[1], (), 0, devices_total)
    position = jnp.arange(devices_total, dtype=jnp.int32)
    return jnp.where(position == filled, SLOT_DEV, counts).astype(jnp.int32)


def set_ends(result, stream_key, least, top_value):
    spot = [jax.random.randint(jax.random.fold_in(stream_key, axis), (), 0, length) for axis, length in enumerate(result.shape)]
    main_axis = result.shape.index(max(result.shape))
    next_to = spot[:main_axis] + [(spot[main_axis] + 1) % result.shape[main_axis]] + spot[main_axis + 1:]
    return result.at[tuple(spot)].set(least).at[tuple(next_to)].set(top_value)


def block_levels(key, shape, cuts, least, largest):
    gain = 1.0
    for axis_at, parts in cuts:
        draws = jax.random.uniform(jax.random.fold_in(jax.random.fold_in(key, 6), axis_at), (parts,), jnp.float32, least / len(cuts), largest / len(cuts))
        gain = gain * jnp.repeat(jnp.exp(draws), shape[axis_at] // parts).reshape((-1,) + (1,) * (len(shape) - 1 - axis_at))
    return gain


def gaussian(key, shape, width, reach, cuts=(), kind=jnp.bfloat16):
    drawn = jax.random.normal(key, shape, jnp.float32) * width
    if len(cuts) > 0:
        drawn = block_levels(key, shape, cuts, -0.22, 0.18) * drawn
    return jnp.clip(drawn, min=-reach, max=reach).astype(kind)


def setup_inputs(seed: int = 0) -> dict:
    key_of = jax.random.split(jax.random.key(seed), 7)
    return {
        "density_history": gaussian(key_of[0], (HISTORY, NZ, NY, NX), 1.0, 6.0, ((1, 8), (2, 4)), jnp.float32),
        "residual_history": draw_residual_history(jax.random.fold_in(key_of[6], 71), 0),
        "occupancy_history": gaussian(key_of[2], (HISTORY, SLOTS, ORBITALS * ORBITALS), 1.0, 6.0, ((1, 32),), jnp.float32),
        "occupancy_residual": gaussian(key_of[3], (HISTORY, SLOTS, ORBITALS * ORBITALS), 1.0, 6.0, ((1, 32),), jnp.float32),
        "species": set_ends(jax.random.randint(key_of[4], (SLOTS,), 0, 4), jax.random.fold_in(key_of[4], 1), 0, 3).astype(jnp.int32),
        "slot_count": draw_slot_count(jax.random.fold_in(key_of[6], 71), 0),
    }


highest = lax.Precision.HIGHEST
grid_mixing = 0.5
block_mixing = 0.5
kerker_wave = 6.0
species_orbitals = (18, 13, 8, 5)

def block_mask(species, slot_count):
    position = jnp.arange(species.shape[0], dtype=jnp.int32)
    owner_count = slot_count[(position // SLOT_DEV).astype(jnp.int32)]
    live = position % SLOT_DEV < owner_count
    orbitals = jnp.zeros_like(species)
    for species_index, orbital_number in enumerate(species_orbitals):
        orbitals = orbitals + orbital_number * (species == species_index).astype(jnp.int32)
    entry = jnp.arange(ORBITALS * ORBITALS, dtype=jnp.int32)
    row_index = entry // ORBITALS
    column_index = entry % ORBITALS
    inside = (row_index[None, :] < orbitals[:, None]) & (column_index[None, :] < orbitals[:, None]) & live[:, None]
    return inside.astype(jnp.float32)

def mixing_weights(intersection):
    factor = jnp.linalg.cholesky(intersection)
    column = jnp.ones((intersection.shape[0], 1), intersection.dtype)
    middle = lax.linalg.triangular_solve(factor, column, left_side=True, lower=True)
    solved = lax.linalg.triangular_solve(factor, middle, left_side=True, lower=True, transpose_a=True)
    return solved[:, 0] / jnp.sum(solved)

def magnitude(length):
    index = jnp.arange(length, dtype=jnp.int32)
    return jnp.minimum(index, length - index).astype(jnp.float32)

def reference(density_history, residual_history, occupancy_history, occupancy_residual, species, slot_count):
    mask = block_mask(species, slot_count)
    flat = residual_history.reshape(HISTORY, -1)
    grid_intersection = jnp.dot(flat, flat.T, precision=highest) / (NX * NY * NZ)
    blocks = (occupancy_residual * mask[None]).reshape(HISTORY, -1)
    block_intersection = jnp.dot(blocks, blocks.T, precision=highest) / (100.0 * SLOTS)
    weights = mixing_weights(grid_intersection + block_intersection)
    mixed = jnp.tensordot(weights, residual_history, axes=1, precision=highest)
    spectrum = jnp.fft.fftn(mixed)
    square = magnitude(NZ)[:, None, None] ** 2 + magnitude(NY)[None, :, None] ** 2 + magnitude(NX)[None, None, :] ** 2
    factor = square / (square + kerker_wave * kerker_wave)
    filtered = jnp.real(jnp.fft.ifftn(spectrum * factor)).astype(jnp.float32)
    new_density = jnp.tensordot(weights, density_history, axes=1, precision=highest) + grid_mixing * filtered
    mixed_blocks = jnp.tensordot(weights, occupancy_history + block_mixing * occupancy_residual, axes=1, precision=highest)
    return (new_density, mask * mixed_blocks)
```

```python
import functools
import math

import jax
import jax.numpy as jnp
import numpy as np
from jax import lax
from jax.experimental import pallas as pl
from jax.experimental.pallas import tpu as pltpu
from jax.sharding import PartitionSpec as P

ORBITALS = 18


highest = lax.Precision.HIGHEST
grid_mixing = 0.5
block_mixing = 0.5
kerker_wave = 6.0
species_orbitals = (18, 13, 8, 5)


def block_mask(species, slot_count):
    live = jnp.arange(species.shape[0], dtype=jnp.int32) < slot_count[0]
    orbitals = jnp.zeros_like(species)
    for species_index, orbital_number in enumerate(species_orbitals):
        orbitals = orbitals + orbital_number * (species == species_index).astype(jnp.int32)
    entry = jnp.arange(ORBITALS * ORBITALS, dtype=jnp.int32)
    row_index = entry // ORBITALS
    column_index = entry % ORBITALS
    inside = (
        (row_index[None, :] < orbitals[:, None])
        & (column_index[None, :] < orbitals[:, None])
        & live[:, None]
    )
    return inside.astype(jnp.float32)


def mixing_weights(intersection):
    factor = jnp.linalg.cholesky(intersection)
    column = jnp.ones((intersection.shape[0], 1), intersection.dtype)
    middle = lax.linalg.triangular_solve(factor, column, left_side=True, lower=True)
    solved = lax.linalg.triangular_solve(
        factor, middle, left_side=True, lower=True, transpose_a=True
    )
    return solved[:, 0] / jnp.sum(solved)


def cosine_sine(length, freq_index, space_index):
    product = freq_index * space_index % length
    angle = 2.0 * math.pi / length * product.astype(jnp.float32)
    return (jnp.cos(angle), jnp.sin(angle))


def forward_spectra(fields, pencil_move, slab_move):
    batches, z_local, y_local, x_length = fields.shape
    pencil_count = lax.axis_size("pencil")
    slab_count = lax.axis_size("slab")
    x_columns = x_length // 2
    kx_local = x_columns // pencil_count
    y_length = y_local * pencil_count
    ky_local = y_length // slab_count
    z_length = z_local * slab_count
    freq_index = jnp.arange(x_columns, dtype=jnp.int32).reshape(pencil_count, kx_local, 1)
    space_index = jnp.arange(x_length, dtype=jnp.int32).reshape(1, 1, x_length)
    cosine, sine = cosine_sine(x_length, freq_index, space_index)
    nyquist = cosine_sine(x_length, jnp.full((1, 1, 1), x_length // 2, jnp.int32), space_index)[0]
    sine = jnp.where(freq_index == 0, -nyquist, sine)
    real_part = jnp.einsum("bzyx,pkx->bpkzy", fields, cosine, precision=highest)
    imag_part = -jnp.einsum("bzyx,pkx->bpkzy", fields, sine, precision=highest)
    packed = jnp.stack((real_part, imag_part), axis=1).reshape(batches, 2, pencil_count, -1)
    moved = pencil_move(packed).reshape(batches, 2, pencil_count, kx_local, z_local, y_local)
    freq_index = jnp.arange(y_length, dtype=jnp.int32).reshape(slab_count, ky_local, 1, 1)
    space_index = jnp.arange(y_length, dtype=jnp.int32).reshape(1, 1, pencil_count, y_local)
    cosine, sine = cosine_sine(y_length, freq_index, space_index)
    real_input = moved[:, 0]
    imag_input = moved[:, 1]
    form = "bskzy,glsy->bgklz"
    real_part = jnp.einsum(form, real_input, cosine, precision=highest) + jnp.einsum(
        form, imag_input, sine, precision=highest
    )
    imag_part = jnp.einsum(form, imag_input, cosine, precision=highest) - jnp.einsum(
        form, real_input, sine, precision=highest
    )
    packed = jnp.stack((real_part, imag_part), axis=1).reshape(batches, 2, slab_count, -1)
    moved = slab_move(packed).reshape(batches, 2, slab_count, kx_local, ky_local, z_local)
    freq_index = jnp.arange(z_length, dtype=jnp.int32).reshape(z_length, 1, 1)
    space_index = jnp.arange(z_length, dtype=jnp.int32).reshape(1, slab_count, z_local)
    cosine, sine = cosine_sine(z_length, freq_index, space_index)
    real_input = moved[:, 0]
    imag_input = moved[:, 1]
    form = "bgklz,mgz->bklm"
    real_part = jnp.einsum(form, real_input, cosine, precision=highest) + jnp.einsum(
        form, imag_input, sine, precision=highest
    )
    imag_part = jnp.einsum(form, imag_input, cosine, precision=highest) - jnp.einsum(
        form, real_input, sine, precision=highest
    )
    return jnp.stack((real_part, imag_part), axis=1)


def magnitude(index, length):
    return jnp.minimum(index, length - index).astype(jnp.float32)


def kerker_factor(freq_x, ky_local, x_length, y_length, z_length):
    freq_y = lax.axis_index("slab") * ky_local + jnp.arange(ky_local, dtype=jnp.int32)
    freq_z = jnp.arange(z_length, dtype=jnp.int32)
    square = (
        magnitude(freq_x, x_length)[:, None, None] ** 2
        + magnitude(freq_y, y_length)[None, :, None] ** 2
        + magnitude(freq_z, z_length)[None, None, :] ** 2
    )
    return square / (square + kerker_wave * kerker_wave)


def inverse_field(spectrum, z_local, y_local, x_length):
    pencil_count = lax.axis_size("pencil")
    slab_count = lax.axis_size("slab")
    x_columns = x_length // 2
    kx_local = x_columns // pencil_count
    slots = spectrum.shape[1]
    y_length = y_local * pencil_count
    ky_local = y_length // slab_count
    z_length = z_local * slab_count
    freq_index = jnp.arange(z_length, dtype=jnp.int32).reshape(z_length, 1, 1)
    space_index = jnp.arange(z_length, dtype=jnp.int32).reshape(1, slab_count, z_local)
    cosine, sine = cosine_sine(z_length, freq_index, space_index)
    real_input = spectrum[0]
    imag_input = spectrum[1]
    form = "klm,mdz->dklz"
    real_part = jnp.einsum(form, real_input, cosine, precision=highest) - jnp.einsum(
        form, imag_input, sine, precision=highest
    )
    imag_part = jnp.einsum(form, real_input, sine, precision=highest) + jnp.einsum(
        form, imag_input, cosine, precision=highest
    )
    packed = jnp.stack((real_part, imag_part), axis=0).reshape(2, slab_count, -1)
    moved = lax.all_to_all(packed, "slab", split_axis=1, concat_axis=1, tiled=True).reshape(
        2, slab_count, slots, ky_local, z_local
    )
    freq_index = jnp.arange(y_length, dtype=jnp.int32).reshape(slab_count, ky_local, 1, 1)
    space_index = jnp.arange(y_length, dtype=jnp.int32).reshape(1, 1, pencil_count, y_local)
    cosine, sine = cosine_sine(y_length, freq_index, space_index)
    real_input = moved[0]
    imag_input = moved[1]
    form = "gklz,glqy->qkzy"
    real_part = jnp.einsum(form, real_input, cosine, precision=highest) - jnp.einsum(
        form, imag_input, sine, precision=highest
    )
    imag_part = jnp.einsum(form, real_input, sine, precision=highest) + jnp.einsum(
        form, imag_input, cosine, precision=highest
    )
    packed = jnp.stack((real_part, imag_part), axis=0).reshape(2, pencil_count, -1)
    moved = lax.all_to_all(packed, "pencil", split_axis=1, concat_axis=1, tiled=True).reshape(
        2, pencil_count, slots, z_local, y_local
    )
    pencil_index = jnp.arange(pencil_count, dtype=jnp.int32).reshape(pencil_count, 1, 1)
    slot_index = jnp.arange(slots, dtype=jnp.int32).reshape(1, slots, 1)
    space_index = jnp.arange(x_length, dtype=jnp.int32).reshape(1, 1, x_length)
    freq_index = pencil_index * kx_local + slot_index
    cosine, sine = cosine_sine(x_length, freq_index, space_index)
    nyquist = cosine_sine(x_length, jnp.full((1, 1, 1), x_length // 2, jnp.int32), space_index)[0]
    ordinary = slot_index < kx_local
    doubling = jnp.where(freq_index == 0, 1.0, 2.0)
    real_table = jnp.where(ordinary, doubling * cosine, 0.0)
    imag_table = jnp.where(ordinary, -doubling * sine, jnp.where(pencil_index == 0, nyquist, 0.0))
    form = "pkzy,pkx->zyx"
    field = jnp.einsum(form, moved[0], real_table, precision=highest) + jnp.einsum(
        form, moved[1], imag_table, precision=highest
    )
    return field / (x_length * y_length * z_length)


def body(
    density_history, residual_history, occupancy_history, occupancy_residual, species, slot_count
):
    histories, z_local, y_local, x_length = residual_history.shape
    slab_count = lax.axis_size("slab")
    pencil_count = lax.axis_size("pencil")
    cell_total = z_local * slab_count * y_local * pencil_count * x_length
    slot_total = species.shape[0] * slab_count * pencil_count
    mask = block_mask(species, slot_count)
    flat = residual_history.reshape(histories, -1)
    grid_local = jnp.dot(flat, flat.T, precision=highest) / cell_total
    blocks = (occupancy_residual * mask[None]).reshape(histories, -1)
    block_local = jnp.dot(blocks, blocks.T, precision=highest) / (100.0 * slot_total)
    grid_intersection, block_intersection = lax.psum((grid_local, block_local), ("slab", "pencil"))
    weights = mixing_weights(grid_intersection + block_intersection)
    mixed = jnp.tensordot(weights, residual_history, axes=1, precision=highest)
    spectrum = forward_spectra(
        mixed[None],
        lambda packed: lax.all_to_all(packed, "pencil", split_axis=2, concat_axis=2, tiled=True),
        lambda packed: lax.all_to_all(packed, "slab", split_axis=2, concat_axis=2, tiled=True),
    )[0]
    x_columns = x_length // 2
    kx_local = x_columns // pencil_count
    y_length = y_local * pencil_count
    z_length = z_local * slab_count
    ky_local = y_length // slab_count
    freq_x = lax.axis_index("pencil") * kx_local + jnp.arange(kx_local, dtype=jnp.int32)
    factor = kerker_factor(freq_x, ky_local, x_length, y_length, z_length)
    filtered_spectrum = spectrum * factor[None]
    nyquist_x = jnp.full((1,), x_length // 2, jnp.int32)
    nyquist_factor = kerker_factor(nyquist_x, ky_local, x_length, y_length, z_length)
    owner = (lax.axis_index("pencil") == 0).astype(jnp.float32)
    extra = spectrum[:, 0:1] * nyquist_factor[None] * owner
    filtered_spectrum = jnp.concatenate((filtered_spectrum, extra), axis=1)
    filtered = inverse_field(filtered_spectrum, z_local, y_local, x_length)
    new_density = (
        jnp.tensordot(weights, density_history, axes=1, precision=highest) + grid_mixing * filtered
    )
    mixed_blocks = jnp.tensordot(
        weights, occupancy_history + block_mixing * occupancy_residual, axes=1, precision=highest
    )
    return (new_density, mask * mixed_blocks)


MESH = pl.DeviceIdType.MESH


def split(value):
    high = value.astype(jnp.bfloat16)
    low = (value - high.astype(jnp.float32)).astype(jnp.bfloat16)
    return high, low


def three(left, right, dims):
    numbers = (dims, ((), ()))
    dot = functools.partial(
        lax.dot_general, dimension_numbers=numbers, preferred_element_type=jnp.float32
    )
    return dot(left[1], right[0]) + dot(left[0], right[1]) + dot(left[0], right[0])


def halves(table):
    table = np.asarray(table, np.float32)
    high = table.astype(jnp.bfloat16)
    low = (table - high.astype(np.float32)).astype(jnp.bfloat16)
    return np.stack((high, low))


def waves(rows, columns, length):
    angle = 2.0 * np.pi / length * (np.outer(rows, columns) % length)
    return np.cos(angle), np.sin(angle)


def tables(x_length, y_length, z_length, pencil_count, lanes):
    columns = x_length // 2
    cosine, sine = waves(np.arange(columns), np.arange(x_length), x_length)
    nyquist = np.where(np.arange(x_length) % 2 == 0, 1.0, -1.0)
    imag = -sine
    imag[0] = nyquist
    x_forward = np.stack((cosine, imag), axis=1).reshape(x_length, x_length)
    doubling = np.where(np.arange(columns) == 0, 1.0, 2.0)[:, None]
    back = np.stack((doubling * cosine, doubling * imag), axis=1).reshape(x_length, x_length)
    x_back = back * (grid_mixing / (x_length * y_length * z_length))
    cosine, sine = waves(np.arange(y_length), np.arange(y_length), y_length)
    y_local = y_length // pencil_count
    y_forward = np.stack((cosine, sine)).reshape(2, pencil_count, y_local, y_length)
    y_back = np.zeros((2, y_length, pencil_count, lanes))
    y_back[:, :, :, :y_local] = np.stack((cosine, sine)).reshape(2, y_length, pencil_count, y_local)
    y_back = y_back.reshape(2, y_length, pencil_count * lanes)
    cosine, sine = waves(np.arange(z_length), np.arange(z_length), z_length)
    z_forward = np.block([[cosine, sine], [-sine, cosine]])
    z_back = np.block([[cosine, -sine], [sine, cosine]])
    return [halves(t) for t in (x_forward, x_back, y_forward, y_back, z_forward, z_back)]


def pairs_of(count):
    return [(i, j) for i in range(count) for j in range(i + 1)]


def solve_weights(entry, count):
    lower, pivot = {}, []
    for j in range(count):
        scaled = [lower[j, k] * pivot[k] for k in range(j)]
        value = entry[j, j]
        for k in range(j):
            value = value - lower[j, k] * scaled[k]
        pivot.append(value)
        for i in range(j + 1, count):
            value = entry[i, j]
            for k in range(j):
                value = value - lower[i, k] * scaled[k]
            lower[i, j] = value / pivot[j]
    middle = []
    for i in range(count):
        value = jnp.ones_like(pivot[0])
        for k in range(i):
            value = value - lower[i, k] * middle[k]
        middle.append(value)
    solved = [None] * count
    for i in reversed(range(count)):
        value = middle[i] / pivot[i]
        for k in range(i + 1, count):
            value = value - lower[k, i] * solved[k]
        solved[i] = value
    total = solved[0]
    for value in solved[1:]:
        total = total + value
    return [value / total for value in solved]


def mix_kernel(
    slabs, pencils, cells, slots,
    res_hbm, dens_hbm, occ_ref, occ_res_ref, limit_ref, corner_ref,
    xf_ref, xb_ref, yf_ref, yb_ref, zf_ref, zb_ref,
    out_ref, occ_out_ref,
    res, dens, sums, mixed, send_box, planes, spectrum, back_box, field,
    load_sem, sum_send, sum_recv, go_send, go_recv, back_send, back_recv,
):
    devices = slabs * pencils
    count, z_local, y_local, x_length = res.shape
    slots_k = x_length // 2 // devices
    freqs = 2 * slots_k
    z_length = z_local * slabs
    y_length = y_local * pencils
    lanes = planes.shape[-1]
    slab = lax.axis_index("slab")
    pencil = lax.axis_index("pencil")
    me = slab * pencils + pencil
    pairs = pairs_of(count)

    def place(index):
        return (lax.div(index, pencils), lax.rem(index, pencils))

    def other(step):
        return lax.rem(me + step, devices)

    barrier = pltpu.get_barrier_semaphore()

    def greet(step, _):
        pl.semaphore_signal(
            barrier, inc=1, device_id=place(other(step)), device_id_type=MESH
        )
        return 0

    lax.fori_loop(1, devices, greet, 0)

    def load(source, target, which, z):
        return pltpu.make_async_copy(source.at[:, z], target.at[:, z], load_sem.at[which, z])

    for z in range(z_local):
        load(res_hbm, res, 0, z).start()
    for z in range(z_local):
        load(dens_hbm, dens, 1, z).start()

    mask = (corner_ref[...] < limit_ref[...]).astype(jnp.float32)
    blocks = [occ_res_ref[i] * mask for i in range(count)]
    totals = [
        jnp.sum(blocks[i] * blocks[j], keepdims=True) / (100.0 * slots) for i, j in pairs
    ]
    whole = x_length // 128
    rest = x_length - whole * 128
    for first, width, tiles in ((0, 128, whole), (whole * 128, rest, 1 if rest else 0)):
        if tiles == 0:
            continue
        acc = [jnp.zeros((8, width), jnp.float32) for _ in pairs]
        for z in range(z_local):
            if first == 0:
                load(res_hbm, res, 0, z).wait()

            def rows(step, acc):
                acc = list(acc)
                row = pl.multiple_of(step * 8, 8)
                for t in range(tiles):
                    lane = first + 128 * t
                    part = [res[i, z, pl.ds(row, 8), lane:lane + width] for i in range(count)]
                    for at, (i, j) in enumerate(pairs):
                        acc[at] = acc[at] + part[i] * part[j]
                return tuple(acc)

            acc = lax.fori_loop(0, y_local // 8, rows, tuple(acc))
        totals = [t + jnp.sum(a, keepdims=True) / cells for t, a in zip(totals, acc)]
    lane_index = lax.broadcasted_iota(jnp.int32, (1, 128), 1)
    packed = jnp.zeros((1, 128), jnp.float32)
    for at, value in enumerate(totals):
        packed = jnp.where(lane_index == at, value, packed)
    sums[me] = packed

    pl.semaphore_wait(barrier, devices - 1)

    def sum_copy(step, source):
        return pltpu.make_async_remote_copy(
            src_ref=sums.at[source], dst_ref=sums.at[source],
            send_sem=sum_send.at[step], recv_sem=sum_recv.at[source],
            device_id=place(other(step)), device_id_type=MESH,
        )

    def start_sum(step, _):
        sum_copy(step, me).start()
        return 0

    def wait_sum(step, _):
        sum_copy(step, other(step)).wait_recv()
        return 0

    def drain_sum(step, _):
        sum_copy(step, me).wait_send()
        return 0

    lax.fori_loop(1, devices, start_sum, 0)
    lax.fori_loop(1, devices, wait_sum, 0)
    gathered = sums[0]
    for d in range(1, devices):
        gathered = gathered + sums[d]
    entry = {
        pair: jnp.sum(jnp.where(lane_index == at, gathered, 0.0), axis=1, keepdims=True)
        for at, pair in enumerate(pairs)
    }
    weights = solve_weights(entry, count)

    x_forward = (xf_ref[0], xf_ref[1])
    mixed[:, y_local:, :] = jnp.zeros((z_local, lanes - y_local, x_length), jnp.float32)
    send_rows = send_box.reshape(devices * freqs * z_local, lanes)
    for z in range(z_local):
        total = weights[0] * res[0, z]
        for i in range(1, count):
            total = total + weights[i] * res[i, z]
        mixed[z, :y_local, :] = total
        send_rows[pl.ds(z, x_length, stride=z_local), :] = three(
            x_forward, split(mixed[z]), ((1,), (1,))
        )

    def go_copy(step, source, target):
        s, p = place(source)
        return pltpu.make_async_remote_copy(
            src_ref=send_box.at[target, :, :, WIDTH],
            dst_ref=planes.at[p, :, pl.ds(pl.multiple_of(s * z_local, z_local), z_local), WIDTH],
            send_sem=go_send.at[step], recv_sem=go_recv.at[source],
            device_id=place(target), device_id_type=MESH,
        )

    def start_go(step, _):
        go_copy(step, me, other(step)).start()
        return 0

    def wait_go(step, _):
        go_copy(step, other(step), other(step)).wait_recv()
        return 0

    def drain_go(step, _):
        go_copy(step, me, other(step)).wait_send()
        return 0

    lax.fori_loop(1, devices, start_go, 0)
    mine = pl.ds(pl.multiple_of(slab * z_local, z_local), z_local)
    planes[pencil, :, mine, :] = send_box[me]

    for z in range(z_local):
        load(dens_hbm, dens, 1, z).wait()
        total = weights[0] * dens[0, z]
        for i in range(1, count):
            total = total + weights[i] * dens[i, z]
        out_ref[z] = total
    total = weights[0] * (occ_ref[0] + block_mixing * occ_res_ref[0])
    for i in range(1, count):
        total = total + weights[i] * (occ_ref[i] + block_mixing * occ_res_ref[i])
    occ_out_ref[...] = mask * total
    lax.fori_loop(1, devices, drain_sum, 0)

    lax.fori_loop(1, devices, wait_go, 0)

    along_cosine, along_sine = None, None
    for p in range(pencils):
        block = split(planes[p].reshape(freqs * z_length, lanes)[:, :y_local])
        cosine = three(block, (yf_ref[0, 0, p], yf_ref[1, 0, p]), ((1,), (0,)))
        sine = three(block, (yf_ref[0, 1, p], yf_ref[1, 1, p]), ((1,), (0,)))
        along_cosine = cosine if p == 0 else along_cosine + cosine
        along_sine = sine if p == 0 else along_sine + sine
    z_forward = (zf_ref[0], zf_ref[1])
    z_back = (zb_ref[0], zb_ref[1])
    shape = (2 * z_length, y_length)
    z_index = lax.rem(lax.broadcasted_iota(jnp.int32, shape, 0), z_length)
    y_index = lax.broadcasted_iota(jnp.int32, shape, 1)
    z_size = jnp.minimum(z_index, z_length - z_index).astype(jnp.float32)
    y_size = jnp.minimum(y_index, y_length - y_index).astype(jnp.float32)
    flat = z_size * z_size + y_size * y_size

    def filtered(wave, freq_x):
        size = freq_x.astype(jnp.float32)
        square = flat + size * size
        return split(wave * (square / (square + kerker_wave * kerker_wave)))

    for k in range(slots_k):
        top, low = 2 * k * z_length, (2 * k + 1) * z_length
        end = low + z_length
        real = along_cosine[top:low] + along_sine[low:end]
        imag = along_cosine[low:end] - along_sine[top:low]
        wave = three(z_forward, split(jnp.concatenate((real, imag), axis=0)), ((1,), (0,)))
        freq_x = me * slots_k + k
        spectrum[k] = three(z_back, filtered(wave, freq_x), ((1,), (0,)))
        if k == 0:
            freq_x = jnp.where(me == 0, x_length // 2, freq_x)
            spectrum[slots_k] = three(z_back, filtered(wave, freq_x), ((1,), (0,)))
    block = split(spectrum[...].reshape((slots_k + 1) * 2 * z_length, y_length))
    along_cosine = three(block, (yb_ref[0, 0], yb_ref[1, 0]), ((1,), (0,)))
    along_sine = three(block, (yb_ref[0, 1], yb_ref[1, 1]), ((1,), (0,)))
    for k in range(slots_k):
        top, low = 2 * k * z_length, (2 * k + 1) * z_length
        end = low + z_length
        real = along_cosine[top:low] - along_sine[low:end]
        if k == 0:
            top, low = 2 * slots_k * z_length, (2 * slots_k + 1) * z_length
            end = low + z_length
        imag = along_cosine[low:end] + along_sine[top:low]
        for p in range(pencils):
            back_box[p, 2 * k] = real[:, p * lanes:(p + 1) * lanes]
            back_box[p, 2 * k + 1] = imag[:, p * lanes:(p + 1) * lanes]

    def back_copy(step, source, target):
        s, p = place(target)
        return pltpu.make_async_remote_copy(
            src_ref=back_box.at[p, :, pl.ds(pl.multiple_of(s * z_local, z_local), z_local), WIDTH],
            dst_ref=field.at[source, :, :, WIDTH],
            send_sem=back_send.at[step], recv_sem=back_recv.at[source],
            device_id=(s, p), device_id_type=MESH,
        )

    def start_back(step, _):
        back_copy(step, me, other(step)).start()
        return 0

    def wait_back(step, _):
        back_copy(step, other(step), other(step)).wait_recv()
        return 0

    def drain_back(step, _):
        back_copy(step, me, other(step)).wait_send()
        return 0

    lax.fori_loop(1, devices, start_back, 0)
    field[me] = back_box[pencil, :, mine, :]
    lax.fori_loop(1, devices, drain_go, 0)
    lax.fori_loop(1, devices, wait_back, 0)
    field_rows = field.reshape(devices * freqs * z_local, lanes)
    x_back = (xb_ref[0], xb_ref[1])
    for z in range(z_local):
        waves_z = split(field_rows[pl.ds(z, x_length, stride=z_local), :])
        out_ref[z] += three(waves_z, x_back, ((0,), (0,)))[:y_local]
    lax.fori_loop(1, devices, drain_back, 0)


WIDTH = slice(None)


def fused_body(
    density_history, residual_history, occupancy_history, occupancy_residual, species, slot_count
):
    count, z_local, y_local, x_length = residual_history.shape
    slabs = lax.axis_size("slab")
    pencils = lax.axis_size("pencil")
    devices = slabs * pencils
    z_length, y_length = z_local * slabs, y_local * pencils
    lanes = -(-y_local // 128) * 128
    freqs = x_length // devices
    live = jnp.arange(species.shape[0], dtype=jnp.int32) < slot_count[0]
    orbitals = jnp.zeros_like(species)
    for species_index, orbital_number in enumerate(species_orbitals):
        orbitals = jnp.where(species == species_index, orbital_number, orbitals)
    limit = jnp.where(live, orbitals, 0)[:, None]
    entry = np.arange(ORBITALS * ORBITALS)
    corner = np.maximum(entry // ORBITALS, entry % ORBITALS)[None].astype(np.int32)
    constants = [
        jnp.asarray(t) for t in tables(x_length, y_length, z_length, pencils, lanes)
    ]
    vmem = pl.BlockSpec(memory_space=pltpu.VMEM)
    hbm = pl.BlockSpec(memory_space=pl.ANY)
    box = (devices, freqs, z_local, lanes)
    plane_box = (pencils, freqs, z_length, lanes)
    sems = pltpu.SemaphoreType.DMA
    return pl.pallas_call(
        functools.partial(
            mix_kernel, slabs, pencils,
            z_length * y_length * x_length, species.shape[0] * devices,
        ),
        out_shape=(
            jax.ShapeDtypeStruct((z_local, y_local, x_length), jnp.float32),
            jax.ShapeDtypeStruct(occupancy_history.shape[1:], jnp.float32),
        ),
        in_specs=[hbm, hbm] + [vmem] * 10,
        out_specs=(vmem, vmem),
        scratch_shapes=[
            pltpu.VMEM(residual_history.shape, jnp.float32),
            pltpu.VMEM(residual_history.shape, jnp.float32),
            pltpu.VMEM((devices, 1, 128), jnp.float32),
            pltpu.VMEM((z_local, lanes, x_length), jnp.float32),
            pltpu.VMEM(box, jnp.float32),
            pltpu.VMEM(plane_box, jnp.float32),
            pltpu.VMEM((freqs // 2 + 1, 2 * z_length, y_length), jnp.float32),
            pltpu.VMEM(plane_box, jnp.float32),
            pltpu.VMEM(box, jnp.float32),
            sems((2, z_local)),
            sems((devices,)), sems((devices,)),
            sems((devices,)), sems((devices,)),
            sems((devices,)), sems((devices,)),
        ],
        compiler_params=pltpu.CompilerParams(
            collective_id=0, has_side_effects=True, vmem_limit_bytes=60000 * 1024
        ),
    )(
        residual_history, density_history, occupancy_history, occupancy_residual,
        limit, jnp.asarray(corner), *constants,
    )


def solution(mesh):
    placed = (
        P(None, "slab", "pencil", None),
        P(None, "slab", "pencil", None),
        P(None, ("slab", "pencil"), None),
        P(None, ("slab", "pencil"), None),
        P(("slab", "pencil")),
        P(("slab", "pencil")),
    )
    devices = mesh.shape["slab"] * mesh.shape["pencil"]

    def chosen(*arrays):
        x_length = arrays[0].shape[3]
        fits = x_length % (2 * devices) == 0 and arrays[0].shape[1] % 8 == 0
        return (fused_body if fits else body)(*arrays)

    return jax.shard_map(
        chosen,
        mesh=mesh,
        in_specs=placed,
        out_specs=(P("slab", "pencil", None), P(("slab", "pencil"), None)),
        check_vma=False,
    )
```

```python
import functools
import math

import jax
import jax.numpy as jnp
import numpy as np
from jax import lax
from jax.experimental import pallas as pl
from jax.experimental.pallas import tpu as pltpu
from jax.sharding import PartitionSpec as P

ORBITALS = 18


highest = lax.Precision.HIGHEST
grid_mixing = 0.5
block_mixing = 0.5
kerker_wave = 6.0
species_orbitals = (18, 13, 8, 5)


def block_mask(species, slot_count):
    live = jnp.arange(species.shape[0], dtype=jnp.int32) < slot_count[0]
    orbitals = jnp.zeros_like(species)
    for species_index, orbital_number in enumerate(species_orbitals):
        orbitals = orbitals + orbital_number * (species == species_index).astype(jnp.int32)
    entry = jnp.arange(ORBITALS * ORBITALS, dtype=jnp.int32)
    row_index = entry // ORBITALS
    column_index = entry % ORBITALS
    inside = (
        (row_index[None, :] < orbitals[:, None])
        & (column_index[None, :] < orbitals[:, None])
        & live[:, None]
    )
    return inside.astype(jnp.float32)


def mixing_weights(intersection):
    factor = jnp.linalg.cholesky(intersection)
    column = jnp.ones((intersection.shape[0], 1), intersection.dtype)
    middle = lax.linalg.triangular_solve(factor, column, left_side=True, lower=True)
    solved = lax.linalg.triangular_solve(
        factor, middle, left_side=True, lower=True, transpose_a=True
    )
    return solved[:, 0] / jnp.sum(solved)


def cosine_sine(length, freq_index, space_index):
    product = freq_index * space_index % length
    angle = 2.0 * math.pi / length * product.astype(jnp.float32)
    return (jnp.cos(angle), jnp.sin(angle))


def forward_spectra(fields, pencil_move, slab_move):
    batches, z_local, y_local, x_length = fields.shape
    pencil_count = lax.axis_size("pencil")
    slab_count = lax.axis_size("slab")
    x_columns = x_length // 2
    kx_local = x_columns // pencil_count
    y_length = y_local * pencil_count
    ky_local = y_length // slab_count
    z_length = z_local * slab_count
    freq_index = jnp.arange(x_columns, dtype=jnp.int32).reshape(pencil_count, kx_local, 1)
    space_index = jnp.arange(x_length, dtype=jnp.int32).reshape(1, 1, x_length)
    cosine, sine = cosine_sine(x_length, freq_index, space_index)
    nyquist = cosine_sine(x_length, jnp.full((1, 1, 1), x_length // 2, jnp.int32), space_index)[0]
    sine = jnp.where(freq_index == 0, -nyquist, sine)
    real_part = jnp.einsum("bzyx,pkx->bpkzy", fields, cosine, precision=highest)
    imag_part = -jnp.einsum("bzyx,pkx->bpkzy", fields, sine, precision=highest)
    packed = jnp.stack((real_part, imag_part), axis=1).reshape(batches, 2, pencil_count, -1)
    moved = pencil_move(packed).reshape(batches, 2, pencil_count, kx_local, z_local, y_local)
    freq_index = jnp.arange(y_length, dtype=jnp.int32).reshape(slab_count, ky_local, 1, 1)
    space_index = jnp.arange(y_length, dtype=jnp.int32).reshape(1, 1, pencil_count, y_local)
    cosine, sine = cosine_sine(y_length, freq_index, space_index)
    real_input = moved[:, 0]
    imag_input = moved[:, 1]
    form = "bskzy,glsy->bgklz"
    real_part = jnp.einsum(form, real_input, cosine, precision=highest) + jnp.einsum(
        form, imag_input, sine, precision=highest
    )
    imag_part = jnp.einsum(form, imag_input, cosine, precision=highest) - jnp.einsum(
        form, real_input, sine, precision=highest
    )
    packed = jnp.stack((real_part, imag_part), axis=1).reshape(batches, 2, slab_count, -1)
    moved = slab_move(packed).reshape(batches, 2, slab_count, kx_local, ky_local, z_local)
    freq_index = jnp.arange(z_length, dtype=jnp.int32).reshape(z_length, 1, 1)
    space_index = jnp.arange(z_length, dtype=jnp.int32).reshape(1, slab_count, z_local)
    cosine, sine = cosine_sine(z_length, freq_index, space_index)
    real_input = moved[:, 0]
    imag_input = moved[:, 1]
    form = "bgklz,mgz->bklm"
    real_part = jnp.einsum(form, real_input, cosine, precision=highest) + jnp.einsum(
        form, imag_input, sine, precision=highest
    )
    imag_part = jnp.einsum(form, imag_input, cosine, precision=highest) - jnp.einsum(
        form, real_input, sine, precision=highest
    )
    return jnp.stack((real_part, imag_part), axis=1)


def magnitude(index, length):
    return jnp.minimum(index, length - index).astype(jnp.float32)


def kerker_factor(freq_x, ky_local, x_length, y_length, z_length):
    freq_y = lax.axis_index("slab") * ky_local + jnp.arange(ky_local, dtype=jnp.int32)
    freq_z = jnp.arange(z_length, dtype=jnp.int32)
    square = (
        magnitude(freq_x, x_length)[:, None, None] ** 2
        + magnitude(freq_y, y_length)[None, :, None] ** 2
        + magnitude(freq_z, z_length)[None, None, :] ** 2
    )
    return square / (square + kerker_wave * kerker_wave)


def inverse_field(spectrum, z_local, y_local, x_length):
    pencil_count = lax.axis_size("pencil")
    slab_count = lax.axis_size("slab")
    x_columns = x_length // 2
    kx_local = x_columns // pencil_count
    slots = spectrum.shape[1]
    y_length = y_local * pencil_count
    ky_local = y_length // slab_count
    z_length = z_local * slab_count
    freq_index = jnp.arange(z_length, dtype=jnp.int32).reshape(z_length, 1, 1)
    space_index = jnp.arange(z_length, dtype=jnp.int32).reshape(1, slab_count, z_local)
    cosine, sine = cosine_sine(z_length, freq_index, space_index)
    real_input = spectrum[0]
    imag_input = spectrum[1]
    form = "klm,mdz->dklz"
    real_part = jnp.einsum(form, real_input, cosine, precision=highest) - jnp.einsum(
        form, imag_input, sine, precision=highest
    )
    imag_part = jnp.einsum(form, real_input, sine, precision=highest) + jnp.einsum(
        form, imag_input, cosine, precision=highest
    )
    packed = jnp.stack((real_part, imag_part), axis=0).reshape(2, slab_count, -1)
    moved = lax.all_to_all(packed, "slab", split_axis=1, concat_axis=1, tiled=True).reshape(
        2, slab_count, slots, ky_local, z_local
    )
    freq_index = jnp.arange(y_length, dtype=jnp.int32).reshape(slab_count, ky_local, 1, 1)
    space_index = jnp.arange(y_length, dtype=jnp.int32).reshape(1, 1, pencil_count, y_local)
    cosine, sine = cosine_sine(y_length, freq_index, space_index)
    real_input = moved[0]
    imag_input = moved[1]
    form = "gklz,glqy->qkzy"
    real_part = jnp.einsum(form, real_input, cosine, precision=highest) - jnp.einsum(
        form, imag_input, sine, precision=highest
    )
    imag_part = jnp.einsum(form, real_input, sine, precision=highest) + jnp.einsum(
        form, imag_input, cosine, precision=highest
    )
    packed = jnp.stack((real_part, imag_part), axis=0).reshape(2, pencil_count, -1)
    moved = lax.all_to_all(packed, "pencil", split_axis=1, concat_axis=1, tiled=True).reshape(
        2, pencil_count, slots, z_local, y_local
    )
    pencil_index = jnp.arange(pencil_count, dtype=jnp.int32).reshape(pencil_count, 1, 1)
    slot_index = jnp.arange(slots, dtype=jnp.int32).reshape(1, slots, 1)
    space_index = jnp.arange(x_length, dtype=jnp.int32).reshape(1, 1, x_length)
    freq_index = pencil_index * kx_local + slot_index
    cosine, sine = cosine_sine(x_length, freq_index, space_index)
    nyquist = cosine_sine(x_length, jnp.full((1, 1, 1), x_length // 2, jnp.int32), space_index)[0]
    ordinary = slot_index < kx_local
    doubling = jnp.where(freq_index == 0, 1.0, 2.0)
    real_table = jnp.where(ordinary, doubling * cosine, 0.0)
    imag_table = jnp.where(ordinary, -doubling * sine, jnp.where(pencil_index == 0, nyquist, 0.0))
    form = "pkzy,pkx->zyx"
    field = jnp.einsum(form, moved[0], real_table, precision=highest) + jnp.einsum(
        form, moved[1], imag_table, precision=highest
    )
    return field / (x_length * y_length * z_length)


def body(
    density_history, residual_history, occupancy_history, occupancy_residual, species, slot_count
):
    histories, z_local, y_local, x_length = residual_history.shape
    slab_count = lax.axis_size("slab")
    pencil_count = lax.axis_size("pencil")
    cell_total = z_local * slab_count * y_local * pencil_count * x_length
    slot_total = species.shape[0] * slab_count * pencil_count
    mask = block_mask(species, slot_count)
    flat = residual_history.reshape(histories, -1)
    grid_local = jnp.dot(flat, flat.T, precision=highest) / cell_total
    blocks = (occupancy_residual * mask[None]).reshape(histories, -1)
    block_local = jnp.dot(blocks, blocks.T, precision=highest) / (100.0 * slot_total)
    grid_intersection, block_intersection = lax.psum((grid_local, block_local), ("slab", "pencil"))
    weights = mixing_weights(grid_intersection + block_intersection)
    mixed = jnp.tensordot(weights, residual_history, axes=1, precision=highest)
    spectrum = forward_spectra(
        mixed[None],
        lambda packed: lax.all_to_all(packed, "pencil", split_axis=2, concat_axis=2, tiled=True),
        lambda packed: lax.all_to_all(packed, "slab", split_axis=2, concat_axis=2, tiled=True),
    )[0]
    x_columns = x_length // 2
    kx_local = x_columns // pencil_count
    y_length = y_local * pencil_count
    z_length = z_local * slab_count
    ky_local = y_length // slab_count
    freq_x = lax.axis_index("pencil") * kx_local + jnp.arange(kx_local, dtype=jnp.int32)
    factor = kerker_factor(freq_x, ky_local, x_length, y_length, z_length)
    filtered_spectrum = spectrum * factor[None]
    nyquist_x = jnp.full((1,), x_length // 2, jnp.int32)
    nyquist_factor = kerker_factor(nyquist_x, ky_local, x_length, y_length, z_length)
    owner = (lax.axis_index("pencil") == 0).astype(jnp.float32)
    extra = spectrum[:, 0:1] * nyquist_factor[None] * owner
    filtered_spectrum = jnp.concatenate((filtered_spectrum, extra), axis=1)
    filtered = inverse_field(filtered_spectrum, z_local, y_local, x_length)
    new_density = (
        jnp.tensordot(weights, density_history, axes=1, precision=highest) + grid_mixing * filtered
    )
    mixed_blocks = jnp.tensordot(
        weights, occupancy_history + block_mixing * occupancy_residual, axes=1, precision=highest
    )
    return (new_density, mask * mixed_blocks)


MESH = pl.DeviceIdType.MESH


def split(value):
    high = value.astype(jnp.bfloat16)
    low = (value - high.astype(jnp.float32)).astype(jnp.bfloat16)
    return high, low


def three(left, right, dims):
    numbers = (dims, ((), ()))
    dot = functools.partial(
        lax.dot_general, dimension_numbers=numbers, preferred_element_type=jnp.float32
    )
    return dot(left[1], right[0]) + dot(left[0], right[1]) + dot(left[0], right[0])


def halves(table):
    table = np.asarray(table, np.float32)
    high = table.astype(jnp.bfloat16)
    low = (table - high.astype(np.float32)).astype(jnp.bfloat16)
    return np.stack((high, low))


def waves(rows, columns, length):
    angle = 2.0 * np.pi / length * (np.outer(rows, columns) % length)
    return np.cos(angle), np.sin(angle)


def tables(x_length, y_length, z_length, pencil_count, slab_count, lanes):
    columns = x_length // 2
    cosine, sine = waves(np.arange(columns), np.arange(x_length), x_length)
    nyquist = np.where(np.arange(x_length) % 2 == 0, 1.0, -1.0)
    imag = -sine
    imag[0] = nyquist
    x_forward = np.stack((cosine, imag), axis=1).reshape(x_length, x_length)
    doubling = np.where(np.arange(columns) == 0, 1.0, 2.0)[:, None]
    back = np.stack((doubling * cosine, doubling * imag), axis=1).reshape(x_length, x_length)
    x_back = back * (grid_mixing / (x_length * y_length * z_length))
    cosine, sine = waves(np.arange(y_length), np.arange(y_length), y_length)
    y_local = y_length // pencil_count
    y_forward = np.stack((cosine, sine)).reshape(2, pencil_count, y_local, y_length)
    y_back = np.zeros((2, y_length, pencil_count, lanes))
    y_back[:, :, :, :y_local] = np.stack((cosine, sine)).reshape(2, y_length, pencil_count, y_local)
    y_back = y_back.reshape(2, y_length, pencil_count * lanes)
    cosine, sine = waves(np.arange(z_length), np.arange(z_length), z_length)
    order = np.arange(z_length).reshape(slab_count, -1).T.reshape(-1)
    cosine, sine = cosine[:, order], sine[:, order]
    z_forward = np.block([[cosine, sine], [-sine, cosine]])
    z_back = np.block([[cosine.T, -sine.T], [sine.T, cosine.T]])
    return [halves(t) for t in (x_forward, x_back, y_forward, y_back, z_forward, z_back)]


def pairs_of(count):
    return [(i, j) for i in range(count) for j in range(i + 1)]


def solve_weights(entry, count):
    lower, pivot = {}, []
    for j in range(count):
        scaled = [lower[j, k] * pivot[k] for k in range(j)]
        value = entry[j, j]
        for k in range(j):
            value = value - lower[j, k] * scaled[k]
        pivot.append(value)
        for i in range(j + 1, count):
            value = entry[i, j]
            for k in range(j):
                value = value - lower[i, k] * scaled[k]
            lower[i, j] = value / pivot[j]
    middle = []
    for i in range(count):
        value = jnp.ones_like(pivot[0])
        for k in range(i):
            value = value - lower[i, k] * middle[k]
        middle.append(value)
    solved = [None] * count
    for i in reversed(range(count)):
        value = middle[i] / pivot[i]
        for k in range(i + 1, count):
            value = value - lower[k, i] * solved[k]
        solved[i] = value
    total = solved[0]
    for value in solved[1:]:
        total = total + value
    return [value / total for value in solved]


def mix_kernel(
    slabs, pencils, cells, slots,
    res_hbm, dens_hbm, occ_ref, occ_res_ref, species_ref, live_ref, corner_ref,
    xf_hbm, yf_hbm, yb_hbm, zf_hbm, zb_hbm,
    out_ref, occ_out_ref, field,
    res, dens, sums, send_box, land_box, planes, spectrum, back_box,
    xf_ref, yf_ref, yb_ref, zf_ref, zb_ref,
    load_sem, table_sem, sum_send, sum_recv, go_send, go_recv, back_send, back_recv,
):
    devices = slabs * pencils
    count, z_local, y_local, x_length = res.shape
    slots_k = x_length // 2 // devices
    freqs = 2 * slots_k
    z_length = z_local * slabs
    y_length = y_local * pencils
    lanes = planes.shape[-1]
    tiles_out = send_box.shape[0]
    slab = lax.axis_index("slab")
    pencil = lax.axis_index("pencil")
    me = slab * pencils + pencil
    pairs = pairs_of(count)

    def place(index):
        return (lax.div(index, pencils), lax.rem(index, pencils))

    def other(step):
        return lax.rem(me + step, devices)

    barrier = pltpu.get_barrier_semaphore()

    def greet(step, _):
        pl.semaphore_signal(
            barrier, inc=1, device_id=place(other(step)), device_id_type=MESH
        )
        return 0

    lax.fori_loop(1, devices, greet, 0)

    def load(source, target, which, z):
        return pltpu.make_async_copy(source.at[:, z], target.at[:, z], load_sem.at[which, z])

    for z in range(z_local):
        load(res_hbm, res, 0, z).start()
    from_tables = (xf_hbm, yf_hbm, zf_hbm, zb_hbm, yb_hbm)
    to_tables = (xf_ref, yf_ref, zf_ref, zb_ref, yb_ref)
    loads = [
        pltpu.make_async_copy(a, b, table_sem.at[at])
        for at, (a, b) in enumerate(zip(from_tables, to_tables))
    ]
    for copy in loads:
        copy.start()
    for z in range(z_local):
        load(dens_hbm, dens, 1, z).start()

    limit_shape = (occ_ref.shape[1], 1)
    slot_index = lax.broadcasted_iota(jnp.int32, limit_shape, 0)
    limit = jnp.zeros(limit_shape, jnp.int32)
    for slot in range(occ_ref.shape[1]):
        orbitals = jnp.int32(0)
        for species_index, orbital_number in enumerate(species_orbitals):
            orbitals = jnp.where(species_ref[slot] == species_index, orbital_number, orbitals)
        orbitals = jnp.where(slot < live_ref[0], orbitals, 0)
        limit = jnp.where(slot_index == slot, orbitals, limit)
    mask = (corner_ref[...] < limit).astype(jnp.float32)
    blocks = [occ_res_ref[i] * mask for i in range(count)]
    totals = [
        jnp.sum(blocks[i] * blocks[j], keepdims=True) / (100.0 * slots) for i, j in pairs
    ]
    whole = x_length // 128
    rest = x_length - whole * 128
    for first, width, tiles in ((0, 128, whole), (whole * 128, rest, 1 if rest else 0)):
        if tiles == 0:
            continue
        acc = [jnp.zeros((8, width), jnp.float32) for _ in pairs]
        for z in range(z_local):
            if first == 0:
                load(res_hbm, res, 0, z).wait()

            def rows(step, acc):
                acc = list(acc)
                row = pl.multiple_of(step * 8, 8)
                for t in range(tiles):
                    lane = first + 128 * t
                    part = [res[i, z, pl.ds(row, 8), lane:lane + width] for i in range(count)]
                    for at, (i, j) in enumerate(pairs):
                        acc[at] = acc[at] + part[i] * part[j]
                return tuple(acc)

            acc = lax.fori_loop(0, y_local // 8, rows, tuple(acc))
        totals = [t + jnp.sum(a, keepdims=True) / cells for t, a in zip(totals, acc)]
    lane_index = lax.broadcasted_iota(jnp.int32, (1, 128), 1)
    packed = jnp.zeros((1, 128), jnp.float32)
    for at, value in enumerate(totals):
        packed = jnp.where(lane_index == at, value, packed)
    sums[me] = packed

    pl.semaphore_wait(barrier, devices - 1)

    def sum_copy(step, source):
        return pltpu.make_async_remote_copy(
            src_ref=sums.at[source], dst_ref=sums.at[source],
            send_sem=sum_send.at[step], recv_sem=sum_recv.at[source],
            device_id=place(other(step)), device_id_type=MESH,
        )

    def start_sum(step, _):
        sum_copy(step, me).start()
        return 0

    def wait_sum(step, _):
        sum_copy(step, other(step)).wait_recv()
        return 0

    def drain_sum(step, _):
        sum_copy(step, me).wait_send()
        return 0

    lax.fori_loop(1, devices, start_sum, 0)
    lax.fori_loop(1, devices, wait_sum, 0)
    gathered = sums[0]
    for d in range(1, devices):
        gathered = gathered + sums[d]
    entry = {
        pair: jnp.sum(jnp.where(lane_index == at, gathered, 0.0), axis=1, keepdims=True)
        for at, pair in enumerate(pairs)
    }
    weights = solve_weights(entry, count)

    loads[0].wait()
    x_forward = (xf_ref[0], xf_ref[1])
    rows_out = z_local * y_local
    mixture = []
    for z in range(z_local):
        total = weights[0] * res[0, z]
        for i in range(1, count):
            total = total + weights[i] * res[i, z]
        mixture.append(total)
    turned = three(x_forward, split(jnp.concatenate(mixture, axis=0)), ((1,), (1,)))
    for t in range(tiles_out):
        send_box[t] = turned[:, t * 128:(t + 1) * 128]

    def share(index):
        return pl.ds(index * freqs, freqs)

    def go_copy(step, source, target):
        return pltpu.make_async_remote_copy(
            src_ref=send_box.at[:, share(target), :],
            dst_ref=land_box.at[:, share(source), :],
            send_sem=go_send.at[step], recv_sem=go_recv.at[source],
            device_id=place(target), device_id_type=MESH,
        )

    def start_go(step, _):
        go_copy(step, me, other(step)).start()
        return 0

    def wait_go(step, _):
        go_copy(step, other(step), other(step)).wait_recv()
        return 0

    def drain_go(step, _):
        go_copy(step, me, other(step)).wait_send()
        return 0

    lax.fori_loop(1, devices, start_go, 0)
    land_box[:, share(me), :] = send_box[:, share(me), :]

    for z in range(z_local):
        load(dens_hbm, dens, 1, z).wait()
        total = weights[0] * dens[0, z]
        for i in range(1, count):
            total = total + weights[i] * dens[i, z]
        out_ref[z * y_local:(z + 1) * y_local, :] = total
    total = weights[0] * (occ_ref[0] + block_mixing * occ_res_ref[0])
    for i in range(1, count):
        total = total + weights[i] * (occ_ref[i] + block_mixing * occ_res_ref[i])
    occ_out_ref[...] = mask * total
    lax.fori_loop(1, devices, drain_sum, 0)

    lax.fori_loop(1, devices, wait_go, 0)

    for copy in loads[1:]:
        copy.wait()
    for p in range(pencils):
        for f in range(freqs):
            parts = [
                land_box[t, pl.ds(p * freqs + f, slabs, stride=pencils * freqs), :]
                for t in range(tiles_out)
            ]
            joined = jnp.concatenate(parts, axis=1)
            for z in range(z_local):
                planes[p, f, z * slabs:(z + 1) * slabs, :y_local] = joined[
                    :, z * y_local:(z + 1) * y_local
                ]

    along_cosine, along_sine = None, None
    for p in range(pencils):
        block = split(planes[p].reshape(freqs * z_length, lanes)[:, :y_local])
        cosine = three(block, (yf_ref[0, 0, p], yf_ref[1, 0, p]), ((1,), (0,)))
        sine = three(block, (yf_ref[0, 1, p], yf_ref[1, 1, p]), ((1,), (0,)))
        along_cosine = cosine if p == 0 else along_cosine + cosine
        along_sine = sine if p == 0 else along_sine + sine
    z_forward = (zf_ref[0], zf_ref[1])
    z_back = (zb_ref[0], zb_ref[1])
    shape = (2 * z_length, y_length)
    z_index = lax.rem(lax.broadcasted_iota(jnp.int32, shape, 0), z_length)
    y_index = lax.broadcasted_iota(jnp.int32, shape, 1)
    z_size = jnp.minimum(z_index, z_length - z_index).astype(jnp.float32)
    y_size = jnp.minimum(y_index, y_length - y_index).astype(jnp.float32)
    flat = z_size * z_size + y_size * y_size

    def filtered(wave, freq_x):
        size = freq_x.astype(jnp.float32)
        square = flat + size * size
        return split(wave * (square / (square + kerker_wave * kerker_wave)))

    for k in range(slots_k):
        top, low = 2 * k * z_length, (2 * k + 1) * z_length
        end = low + z_length
        real = along_cosine[top:low] + along_sine[low:end]
        imag = along_cosine[low:end] - along_sine[top:low]
        wave = three(z_forward, split(jnp.concatenate((real, imag), axis=0)), ((1,), (0,)))
        freq_x = me * slots_k + k
        spectrum[k] = three(z_back, filtered(wave, freq_x), ((1,), (0,)))
        if k == 0:
            freq_x = jnp.where(me == 0, x_length // 2, freq_x)
            spectrum[slots_k] = three(z_back, filtered(wave, freq_x), ((1,), (0,)))
    block = split(spectrum[...].reshape((slots_k + 1) * 2 * z_length, y_length))
    along_cosine = three(block, (yb_ref[0, 0], yb_ref[1, 0]), ((1,), (0,)))
    along_sine = three(block, (yb_ref[0, 1], yb_ref[1, 1]), ((1,), (0,)))
    for k in range(slots_k):
        top, low = 2 * k * z_length, (2 * k + 1) * z_length
        end = low + z_length
        real = along_cosine[top:low] - along_sine[low:end]
        if k == 0:
            top, low = 2 * slots_k * z_length, (2 * slots_k + 1) * z_length
            end = low + z_length
        imag = along_cosine[low:end] + along_sine[top:low]
        for c, part in enumerate((real, imag)):
            for p in range(pencils):
                joined = jnp.concatenate(
                    [
                        part[z * slabs:(z + 1) * slabs, p * lanes:p * lanes + y_local]
                        for z in range(z_local)
                    ],
                    axis=1,
                )
                start = p * freqs + 2 * k + c
                for t in range(tiles_out):
                    back_box[t, pl.ds(start, slabs, stride=pencils * freqs), :] = joined[
                        :, t * 128:(t + 1) * 128
                    ]

    def back_copy(step, source, target):
        return pltpu.make_async_remote_copy(
            src_ref=back_box.at[:, share(target), :],
            dst_ref=field.at[:, share(source), :],
            send_sem=back_send.at[step], recv_sem=back_recv.at[source],
            device_id=place(target), device_id_type=MESH,
        )

    def start_back(step, _):
        back_copy(step, me, other(step)).start()
        return 0

    def wait_back(step, _):
        back_copy(step, other(step), other(step)).wait_recv()
        return 0

    def drain_back(step, _):
        back_copy(step, me, other(step)).wait_send()
        return 0

    lax.fori_loop(1, devices, start_back, 0)
    field[:, share(me), :] = back_box[:, share(me), :]
    lax.fori_loop(1, devices, drain_go, 0)
    lax.fori_loop(1, devices, wait_back, 0)
    lax.fori_loop(1, devices, drain_back, 0)


def finish_kernel(field_ref, dens_ref, occ_ref, xb_ref, out_ref, occ_out_ref):
    x_back = (xb_ref[0], xb_ref[1])
    occ_out_ref[...] = occ_ref[...]
    for t in range(field_ref.shape[0]):
        rows = slice(t * 128, (t + 1) * 128)
        out_ref[rows, :] = dens_ref[rows, :] + three(split(field_ref[t]), x_back, ((0,), (0,)))


def fused_body(
    density_history, residual_history, occupancy_history, occupancy_residual, species, slot_count
):
    count, z_local, y_local, x_length = residual_history.shape
    slabs = lax.axis_size("slab")
    pencils = lax.axis_size("pencil")
    devices = slabs * pencils
    z_length, y_length = z_local * slabs, y_local * pencils
    lanes = -(-y_local // 128) * 128
    freqs = x_length // devices
    entry = np.arange(ORBITALS * ORBITALS)
    corner = np.maximum(entry // ORBITALS, entry % ORBITALS)[None].astype(np.int32)
    x_forward, x_back, *others = [
        jnp.asarray(t) for t in tables(x_length, y_length, z_length, pencils, slabs, lanes)
    ]
    constants = [x_forward, *others]
    vmem = pl.BlockSpec(memory_space=pltpu.VMEM)
    smem = pl.BlockSpec(memory_space=pltpu.SMEM)
    hbm = pl.BlockSpec(memory_space=pltpu.HBM)
    box = (z_local * y_local // 128, devices * freqs, 128)
    sems = pltpu.SemaphoreType.DMA
    flat = jax.ShapeDtypeStruct((z_local * y_local, x_length), jnp.float32)
    blocks = jax.ShapeDtypeStruct(occupancy_history.shape[1:], jnp.float32)
    mixed, mixed_blocks, field = pl.pallas_call(
        functools.partial(
            mix_kernel, slabs, pencils,
            z_length * y_length * x_length, species.shape[0] * devices,
        ),
        out_shape=(flat, blocks, jax.ShapeDtypeStruct(box, jnp.float32)),
        in_specs=[hbm, hbm, vmem, vmem, smem, smem, vmem] + [hbm] * 5,
        out_specs=(vmem, vmem, vmem),
        scratch_shapes=[
            pltpu.VMEM(residual_history.shape, jnp.float32),
            pltpu.VMEM(residual_history.shape, jnp.float32),
            pltpu.VMEM((devices, 1, 128), jnp.float32),
            pltpu.VMEM(box, jnp.float32),
            pltpu.VMEM(box, jnp.float32),
            pltpu.VMEM((pencils, freqs, z_length, lanes), jnp.float32),
            pltpu.VMEM((freqs // 2 + 1, 2 * z_length, y_length), jnp.float32),
            pltpu.VMEM(box, jnp.float32),
            *[pltpu.VMEM(t.shape, t.dtype) for t in constants],
            sems((2, z_local)),
            sems((len(constants),)),
            sems((devices,)), sems((devices,)),
            sems((devices,)), sems((devices,)),
            sems((devices,)), sems((devices,)),
        ],
        compiler_params=pltpu.CompilerParams(
            collective_id=0, has_side_effects=True, vmem_limit_bytes=52000 * 1024
        ),
    )(
        residual_history, density_history, occupancy_history, occupancy_residual,
        species, slot_count, jnp.asarray(corner), *constants,
    )
    new_density, new_blocks = pl.pallas_call(
        finish_kernel,
        out_shape=(flat, blocks),
        in_specs=[vmem] * 4,
        out_specs=(vmem, vmem),
        compiler_params=pltpu.CompilerParams(vmem_limit_bytes=20000 * 1024),
    )(field, mixed, mixed_blocks, x_back)
    return new_density.reshape(z_local, y_local, x_length), new_blocks


def solution(mesh):
    placed = (
        P(None, "slab", "pencil", None),
        P(None, "slab", "pencil", None),
        P(None, ("slab", "pencil"), None),
        P(None, ("slab", "pencil"), None),
        P(("slab", "pencil")),
        P(("slab", "pencil")),
    )
    devices = mesh.shape["slab"] * mesh.shape["pencil"]

    def chosen(*arrays):
        x_length = arrays[0].shape[3]
        _, z_local, y_local, _ = arrays[0].shape
        fits = (
            x_length % (2 * devices) == 0
            and mesh.shape["slab"] % 8 == 0
            and y_local % 16 == 0
            and z_local * y_local % 128 == 0
        )
        return (fused_body if fits else body)(*arrays)

    return jax.shard_map(
        chosen,
        mesh=mesh,
        in_specs=placed,
        out_specs=(P("slab", "pencil", None), P(("slab", "pencil"), None)),
        check_vma=False,
    )
```

```python
import functools
import math

import jax
import jax.numpy as jnp
import numpy as np
from jax import lax
from jax.experimental import pallas as pl
from jax.experimental.pallas import tpu as pltpu
from jax.sharding import PartitionSpec as P

ORBITALS = 18


highest = lax.Precision.HIGHEST
grid_mixing = 0.5
block_mixing = 0.5
kerker_wave = 6.0
species_orbitals = (18, 13, 8, 5)


def block_mask(species, slot_count):
    live = jnp.arange(species.shape[0], dtype=jnp.int32) < slot_count[0]
    orbitals = jnp.zeros_like(species)
    for species_index, orbital_number in enumerate(species_orbitals):
        orbitals = orbitals + orbital_number * (species == species_index).astype(jnp.int32)
    entry = jnp.arange(ORBITALS * ORBITALS, dtype=jnp.int32)
    row_index = entry // ORBITALS
    column_index = entry % ORBITALS
    inside = (
        (row_index[None, :] < orbitals[:, None])
        & (column_index[None, :] < orbitals[:, None])
        & live[:, None]
    )
    return inside.astype(jnp.float32)


def mixing_weights(intersection):
    factor = jnp.linalg.cholesky(intersection)
    column = jnp.ones((intersection.shape[0], 1), intersection.dtype)
    middle = lax.linalg.triangular_solve(factor, column, left_side=True, lower=True)
    solved = lax.linalg.triangular_solve(
        factor, middle, left_side=True, lower=True, transpose_a=True
    )
    return solved[:, 0] / jnp.sum(solved)


def cosine_sine(length, freq_index, space_index):
    product = freq_index * space_index % length
    angle = 2.0 * math.pi / length * product.astype(jnp.float32)
    return (jnp.cos(angle), jnp.sin(angle))


def forward_spectra(fields, pencil_move, slab_move):
    batches, z_local, y_local, x_length = fields.shape
    pencil_count = lax.axis_size("pencil")
    slab_count = lax.axis_size("slab")
    x_columns = x_length // 2
    kx_local = x_columns // pencil_count
    y_length = y_local * pencil_count
    ky_local = y_length // slab_count
    z_length = z_local * slab_count
    freq_index = jnp.arange(x_columns, dtype=jnp.int32).reshape(pencil_count, kx_local, 1)
    space_index = jnp.arange(x_length, dtype=jnp.int32).reshape(1, 1, x_length)
    cosine, sine = cosine_sine(x_length, freq_index, space_index)
    nyquist = cosine_sine(x_length, jnp.full((1, 1, 1), x_length // 2, jnp.int32), space_index)[0]
    sine = jnp.where(freq_index == 0, -nyquist, sine)
    real_part = jnp.einsum("bzyx,pkx->bpkzy", fields, cosine, precision=highest)
    imag_part = -jnp.einsum("bzyx,pkx->bpkzy", fields, sine, precision=highest)
    packed = jnp.stack((real_part, imag_part), axis=1).reshape(batches, 2, pencil_count, -1)
    moved = pencil_move(packed).reshape(batches, 2, pencil_count, kx_local, z_local, y_local)
    freq_index = jnp.arange(y_length, dtype=jnp.int32).reshape(slab_count, ky_local, 1, 1)
    space_index = jnp.arange(y_length, dtype=jnp.int32).reshape(1, 1, pencil_count, y_local)
    cosine, sine = cosine_sine(y_length, freq_index, space_index)
    real_input = moved[:, 0]
    imag_input = moved[:, 1]
    form = "bskzy,glsy->bgklz"
    real_part = jnp.einsum(form, real_input, cosine, precision=highest) + jnp.einsum(
        form, imag_input, sine, precision=highest
    )
    imag_part = jnp.einsum(form, imag_input, cosine, precision=highest) - jnp.einsum(
        form, real_input, sine, precision=highest
    )
    packed = jnp.stack((real_part, imag_part), axis=1).reshape(batches, 2, slab_count, -1)
    moved = slab_move(packed).reshape(batches, 2, slab_count, kx_local, ky_local, z_local)
    freq_index = jnp.arange(z_length, dtype=jnp.int32).reshape(z_length, 1, 1)
    space_index = jnp.arange(z_length, dtype=jnp.int32).reshape(1, slab_count, z_local)
    cosine, sine = cosine_sine(z_length, freq_index, space_index)
    real_input = moved[:, 0]
    imag_input = moved[:, 1]
    form = "bgklz,mgz->bklm"
    real_part = jnp.einsum(form, real_input, cosine, precision=highest) + jnp.einsum(
        form, imag_input, sine, precision=highest
    )
    imag_part = jnp.einsum(form, imag_input, cosine, precision=highest) - jnp.einsum(
        form, real_input, sine, precision=highest
    )
    return jnp.stack((real_part, imag_part), axis=1)


def magnitude(index, length):
    return jnp.minimum(index, length - index).astype(jnp.float32)


def kerker_factor(freq_x, ky_local, x_length, y_length, z_length):
    freq_y = lax.axis_index("slab") * ky_local + jnp.arange(ky_local, dtype=jnp.int32)
    freq_z = jnp.arange(z_length, dtype=jnp.int32)
    square = (
        magnitude(freq_x, x_length)[:, None, None] ** 2
        + magnitude(freq_y, y_length)[None, :, None] ** 2
        + magnitude(freq_z, z_length)[None, None, :] ** 2
    )
    return square / (square + kerker_wave * kerker_wave)


def inverse_field(spectrum, z_local, y_local, x_length):
    pencil_count = lax.axis_size("pencil")
    slab_count = lax.axis_size("slab")
    x_columns = x_length // 2
    kx_local = x_columns // pencil_count
    slots = spectrum.shape[1]
    y_length = y_local * pencil_count
    ky_local = y_length // slab_count
    z_length = z_local * slab_count
    freq_index = jnp.arange(z_length, dtype=jnp.int32).reshape(z_length, 1, 1)
    space_index = jnp.arange(z_length, dtype=jnp.int32).reshape(1, slab_count, z_local)
    cosine, sine = cosine_sine(z_length, freq_index, space_index)
    real_input = spectrum[0]
    imag_input = spectrum[1]
    form = "klm,mdz->dklz"
    real_part = jnp.einsum(form, real_input, cosine, precision=highest) - jnp.einsum(
        form, imag_input, sine, precision=highest
    )
    imag_part = jnp.einsum(form, real_input, sine, precision=highest) + jnp.einsum(
        form, imag_input, cosine, precision=highest
    )
    packed = jnp.stack((real_part, imag_part), axis=0).reshape(2, slab_count, -1)
    moved = lax.all_to_all(packed, "slab", split_axis=1, concat_axis=1, tiled=True).reshape(
        2, slab_count, slots, ky_local, z_local
    )
    freq_index = jnp.arange(y_length, dtype=jnp.int32).reshape(slab_count, ky_local, 1, 1)
    space_index = jnp.arange(y_length, dtype=jnp.int32).reshape(1, 1, pencil_count, y_local)
    cosine, sine = cosine_sine(y_length, freq_index, space_index)
    real_input = moved[0]
    imag_input = moved[1]
    form = "gklz,glqy->qkzy"
    real_part = jnp.einsum(form, real_input, cosine, precision=highest) - jnp.einsum(
        form, imag_input, sine, precision=highest
    )
    imag_part = jnp.einsum(form, real_input, sine, precision=highest) + jnp.einsum(
        form, imag_input, cosine, precision=highest
    )
    packed = jnp.stack((real_part, imag_part), axis=0).reshape(2, pencil_count, -1)
    moved = lax.all_to_all(packed, "pencil", split_axis=1, concat_axis=1, tiled=True).reshape(
        2, pencil_count, slots, z_local, y_local
    )
    pencil_index = jnp.arange(pencil_count, dtype=jnp.int32).reshape(pencil_count, 1, 1)
    slot_index = jnp.arange(slots, dtype=jnp.int32).reshape(1, slots, 1)
    space_index = jnp.arange(x_length, dtype=jnp.int32).reshape(1, 1, x_length)
    freq_index = pencil_index * kx_local + slot_index
    cosine, sine = cosine_sine(x_length, freq_index, space_index)
    nyquist = cosine_sine(x_length, jnp.full((1, 1, 1), x_length // 2, jnp.int32), space_index)[0]
    ordinary = slot_index < kx_local
    doubling = jnp.where(freq_index == 0, 1.0, 2.0)
    real_table = jnp.where(ordinary, doubling * cosine, 0.0)
    imag_table = jnp.where(ordinary, -doubling * sine, jnp.where(pencil_index == 0, nyquist, 0.0))
    form = "pkzy,pkx->zyx"
    field = jnp.einsum(form, moved[0], real_table, precision=highest) + jnp.einsum(
        form, moved[1], imag_table, precision=highest
    )
    return field / (x_length * y_length * z_length)


def body(
    density_history, residual_history, occupancy_history, occupancy_residual, species, slot_count
):
    histories, z_local, y_local, x_length = residual_history.shape
    slab_count = lax.axis_size("slab")
    pencil_count = lax.axis_size("pencil")
    cell_total = z_local * slab_count * y_local * pencil_count * x_length
    slot_total = species.shape[0] * slab_count * pencil_count
    mask = block_mask(species, slot_count)
    flat = residual_history.reshape(histories, -1)
    grid_local = jnp.dot(flat, flat.T, precision=highest) / cell_total
    blocks = (occupancy_residual * mask[None]).reshape(histories, -1)
    block_local = jnp.dot(blocks, blocks.T, precision=highest) / (100.0 * slot_total)
    grid_intersection, block_intersection = lax.psum((grid_local, block_local), ("slab", "pencil"))
    weights = mixing_weights(grid_intersection + block_intersection)
    mixed = jnp.tensordot(weights, residual_history, axes=1, precision=highest)
    spectrum = forward_spectra(
        mixed[None],
        lambda packed: lax.all_to_all(packed, "pencil", split_axis=2, concat_axis=2, tiled=True),
        lambda packed: lax.all_to_all(packed, "slab", split_axis=2, concat_axis=2, tiled=True),
    )[0]
    x_columns = x_length // 2
    kx_local = x_columns // pencil_count
    y_length = y_local * pencil_count
    z_length = z_local * slab_count
    ky_local = y_length // slab_count
    freq_x = lax.axis_index("pencil") * kx_local + jnp.arange(kx_local, dtype=jnp.int32)
    factor = kerker_factor(freq_x, ky_local, x_length, y_length, z_length)
    filtered_spectrum = spectrum * factor[None]
    nyquist_x = jnp.full((1,), x_length // 2, jnp.int32)
    nyquist_factor = kerker_factor(nyquist_x, ky_local, x_length, y_length, z_length)
    owner = (lax.axis_index("pencil") == 0).astype(jnp.float32)
    extra = spectrum[:, 0:1] * nyquist_factor[None] * owner
    filtered_spectrum = jnp.concatenate((filtered_spectrum, extra), axis=1)
    filtered = inverse_field(filtered_spectrum, z_local, y_local, x_length)
    new_density = (
        jnp.tensordot(weights, density_history, axes=1, precision=highest) + grid_mixing * filtered
    )
    mixed_blocks = jnp.tensordot(
        weights, occupancy_history + block_mixing * occupancy_residual, axes=1, precision=highest
    )
    return (new_density, mask * mixed_blocks)


MESH = pl.DeviceIdType.MESH


def split(value):
    high = value.astype(jnp.bfloat16)
    low = (value - high.astype(jnp.float32)).astype(jnp.bfloat16)
    return high, low


def three(left, right, dims):
    numbers = (dims, ((), ()))
    dot = functools.partial(
        lax.dot_general, dimension_numbers=numbers, preferred_element_type=jnp.float32
    )
    return dot(left[1], right[0]) + dot(left[0], right[1]) + dot(left[0], right[0])


def halves(table):
    table = np.asarray(table, np.float32)
    high = table.astype(jnp.bfloat16)
    low = (table - high.astype(np.float32)).astype(jnp.bfloat16)
    return np.stack((high, low))


def waves(rows, columns, length):
    angle = 2.0 * np.pi / length * (np.outer(rows, columns) % length)
    return np.cos(angle), np.sin(angle)


def tables(x_length, y_length, z_length, pencil_count, slab_count):
    columns = x_length // 2
    cosine, sine = waves(np.arange(columns), np.arange(x_length), x_length)
    nyquist = np.where(np.arange(x_length) % 2 == 0, 1.0, -1.0)
    imag = -sine
    imag[0] = nyquist
    slots_k = columns // (pencil_count * slab_count)
    owner, slot = np.arange(columns) // slots_k, np.arange(columns) % slots_k
    chunk = np.searchsorted(cuts_of(slots_k), slot, side="right")
    order = np.lexsort((slot, owner, chunk))
    x_forward = np.stack((cosine, imag), axis=1)[order].reshape(x_length, x_length)
    doubling = np.where(np.arange(columns) == 0, 1.0, 2.0)[:, None]
    back = np.stack((doubling * cosine, doubling * imag), axis=1)[order]
    back = back.reshape(x_length, x_length)
    x_back = back * (grid_mixing / (x_length * y_length * z_length))
    cosine, sine = waves(np.arange(y_length), np.arange(y_length), y_length)
    along_y = np.stack((cosine, sine))
    cosine, sine = waves(np.arange(z_length), np.arange(z_length), z_length)
    order = np.arange(z_length).reshape(slab_count, -1).T.reshape(-1)
    cosine, sine = cosine[:, order], sine[:, order]
    z_forward = np.block([[cosine, sine], [-sine, cosine]])
    z_back = np.block([[cosine.T, -sine.T], [sine.T, cosine.T]])
    return [halves(t) for t in (x_forward, x_back, along_y, z_forward, z_back)]


def cuts_of(slots):
    return [at for at in range(1, slots, 2)] + [slots]


def pairs_of(count):
    return [(i, j) for i in range(count) for j in range(i + 1)]


def solve_weights(entry, count):
    lower, pivot = {}, []
    for j in range(count):
        scaled = [lower[j, k] * pivot[k] for k in range(j)]
        value = entry[j, j]
        for k in range(j):
            value = value - lower[j, k] * scaled[k]
        pivot.append(value)
        for i in range(j + 1, count):
            value = entry[i, j]
            for k in range(j):
                value = value - lower[i, k] * scaled[k]
            lower[i, j] = value / pivot[j]
    middle = []
    for i in range(count):
        value = jnp.ones_like(pivot[0])
        for k in range(i):
            value = value - lower[i, k] * middle[k]
        middle.append(value)
    solved = [None] * count
    for i in reversed(range(count)):
        value = middle[i] / pivot[i]
        for k in range(i + 1, count):
            value = value - lower[k, i] * solved[k]
        solved[i] = value
    total = solved[0]
    for value in solved[1:]:
        total = total + value
    return [value / total for value in solved]


def mix_kernel(
    slabs, pencils, cells, slots,
    res_hbm, dens_hbm, occ_ref, occ_res_ref, species_ref, live_ref, corner_ref,
    xf_hbm, yt_hbm, zf_hbm, zb_hbm,
    out_ref, occ_out_ref, field,
    res, dens, sums, send_box, land_box, planes, spectrum, back_box,
    xf_ref, yt_ref, zf_ref, zb_ref,
    load_sem, table_sem, sum_send, sum_recv, go_send, go_recv, back_send, back_recv,
):
    devices = slabs * pencils
    count, z_local, y_local, x_length = res.shape
    slots_k = x_length // 2 // devices
    freqs = 2 * slots_k
    z_length = z_local * slabs
    y_length = y_local * pencils
    tiles_out = send_box.shape[0]
    slab = lax.axis_index("slab")
    pencil = lax.axis_index("pencil")
    me = slab * pencils + pencil
    pairs = pairs_of(count)

    def place(index):
        return (lax.div(index, pencils), lax.rem(index, pencils))

    def other(step):
        return lax.rem(me + step, devices)

    barrier = pltpu.get_barrier_semaphore()

    def greet(step, _):
        pl.semaphore_signal(
            barrier, inc=1, device_id=place(other(step)), device_id_type=MESH
        )
        return 0

    lax.fori_loop(1, devices, greet, 0)

    def load(source, target, which, z):
        return pltpu.make_async_copy(source.at[:, z], target.at[:, z], load_sem.at[which, z])

    for z in range(z_local):
        load(res_hbm, res, 0, z).start()
    from_tables = (xf_hbm, yt_hbm, zf_hbm, zb_hbm)
    to_tables = (xf_ref, yt_ref, zf_ref, zb_ref)
    loads = [
        pltpu.make_async_copy(a, b, table_sem.at[at])
        for at, (a, b) in enumerate(zip(from_tables, to_tables))
    ]
    for copy in loads:
        copy.start()
    for z in range(z_local):
        load(dens_hbm, dens, 1, z).start()

    limit_shape = (occ_ref.shape[1], 1)
    slot_index = lax.broadcasted_iota(jnp.int32, limit_shape, 0)
    limit = jnp.zeros(limit_shape, jnp.int32)
    for slot in range(occ_ref.shape[1]):
        orbitals = jnp.int32(0)
        for species_index, orbital_number in enumerate(species_orbitals):
            orbitals = jnp.where(species_ref[slot] == species_index, orbital_number, orbitals)
        orbitals = jnp.where(slot < live_ref[0], orbitals, 0)
        limit = jnp.where(slot_index == slot, orbitals, limit)
    mask = (corner_ref[...] < limit).astype(jnp.float32)
    blocks = [occ_res_ref[i] * mask for i in range(count)]
    totals = [
        jnp.sum(blocks[i] * blocks[j], keepdims=True) / (100.0 * slots) for i, j in pairs
    ]
    whole = x_length // 128
    rest = x_length - whole * 128
    for first, width, tiles in ((0, 128, whole), (whole * 128, rest, 1 if rest else 0)):
        if tiles == 0:
            continue
        acc = [jnp.zeros((8, width), jnp.float32) for _ in pairs]
        for z in range(z_local):
            if first == 0:
                load(res_hbm, res, 0, z).wait()

            def rows(step, acc):
                acc = list(acc)
                row = pl.multiple_of(step * 8, 8)
                for t in range(tiles):
                    lane = first + 128 * t
                    part = [res[i, z, pl.ds(row, 8), lane:lane + width] for i in range(count)]
                    for at, (i, j) in enumerate(pairs):
                        acc[at] = acc[at] + part[i] * part[j]
                return tuple(acc)

            acc = lax.fori_loop(0, y_local // 8, rows, tuple(acc))
        totals = [t + jnp.sum(a, keepdims=True) / cells for t, a in zip(totals, acc)]
    lane_index = lax.broadcasted_iota(jnp.int32, (1, 128), 1)
    packed = jnp.zeros((1, 128), jnp.float32)
    for at, value in enumerate(totals):
        packed = jnp.where(lane_index == at, value, packed)
    sums[me] = packed

    pl.semaphore_wait(barrier, devices - 1)

    def sum_copy(step, source):
        return pltpu.make_async_remote_copy(
            src_ref=sums.at[source], dst_ref=sums.at[source],
            send_sem=sum_send.at[step], recv_sem=sum_recv.at[source],
            device_id=place(other(step)), device_id_type=MESH,
        )

    def start_sum(step, _):
        sum_copy(step, me).start()
        return 0

    def wait_sum(step, _):
        sum_copy(step, other(step)).wait_recv()
        return 0

    def drain_sum(step, _):
        sum_copy(step, me).wait_send()
        return 0

    lax.fori_loop(1, devices, start_sum, 0)
    lax.fori_loop(1, devices, wait_sum, 0)
    gathered = sums[0]
    for d in range(1, devices):
        gathered = gathered + sums[d]
    entry = {
        pair: jnp.sum(jnp.where(lane_index == at, gathered, 0.0), axis=1, keepdims=True)
        for at, pair in enumerate(pairs)
    }
    weights = solve_weights(entry, count)

    loads[0].wait()
    mixture = []
    for z in range(z_local):
        total = weights[0] * res[0, z]
        for i in range(1, count):
            total = total + weights[i] * res[i, z]
        mixture.append(total)
    mixture = split(jnp.concatenate(mixture, axis=0))
    ends = cuts_of(slots_k)
    chunks = list(zip([0] + ends[:-1], ends))

    def share(chunk, index):
        first, end = chunks[chunk]
        size = 2 * (end - first)
        return pl.ds(2 * first * devices + index * size, size)

    def go_copy(chunk, step, source, target):
        return pltpu.make_async_remote_copy(
            src_ref=send_box.at[:, share(chunk, target), :],
            dst_ref=land_box.at[:, share(chunk, source), :],
            send_sem=go_send.at[chunk, step], recv_sem=go_recv.at[chunk, source],
            device_id=place(target), device_id_type=MESH,
        )

    def back_copy(chunk, step, source, target):
        return pltpu.make_async_remote_copy(
            src_ref=back_box.at[:, share(chunk, target), :],
            dst_ref=field.at[:, share(chunk, source), :],
            send_sem=back_send.at[chunk, step], recv_sem=back_recv.at[chunk, source],
            device_id=place(target), device_id_type=MESH,
        )

    def start_all(copy, chunk):
        def start(step, _):
            copy(chunk, step, me, other(step)).start()
            return 0

        lax.fori_loop(1, devices, start, 0)

    def land_all(copy, chunk):
        def wait(step, _):
            copy(chunk, step, other(step), other(step)).wait_recv()
            return 0

        lax.fori_loop(1, devices, wait, 0)

    def drain_all(copy, chunk):
        def wait(step, _):
            copy(chunk, step, me, other(step)).wait_send()
            return 0

        lax.fori_loop(1, devices, wait, 0)

    for chunk, (first, end) in enumerate(chunks):
        rows = slice(2 * first * devices, 2 * end * devices)
        turned = three((xf_ref[0, rows, :], xf_ref[1, rows, :]), mixture, ((1,), (1,)))
        for t in range(tiles_out):
            send_box[t, rows, :] = turned[:, t * 128:(t + 1) * 128]
        start_all(go_copy, chunk)
        land_box[:, share(chunk, me), :] = send_box[:, share(chunk, me), :]

    for z in range(z_local):
        load(dens_hbm, dens, 1, z).wait()
        total = weights[0] * dens[0, z]
        for i in range(1, count):
            total = total + weights[i] * dens[i, z]
        out_ref[z * y_local:(z + 1) * y_local, :] = total
    total = weights[0] * (occ_ref[0] + block_mixing * occ_res_ref[0])
    for i in range(1, count):
        total = total + weights[i] * (occ_ref[i] + block_mixing * occ_res_ref[i])
    occ_out_ref[...] = mask * total
    lax.fori_loop(1, devices, drain_sum, 0)

    for copy in loads[1:]:
        copy.wait()
    z_forward = (zf_ref[0], zf_ref[1])
    z_back = (zb_ref[0], zb_ref[1])
    y_cosine = (yt_ref[0, 0], yt_ref[1, 0])
    y_sine = (yt_ref[0, 1], yt_ref[1, 1])
    shape = (2 * z_length, y_length)
    z_index = lax.rem(lax.broadcasted_iota(jnp.int32, shape, 0), z_length)
    y_index = lax.broadcasted_iota(jnp.int32, shape, 1)
    z_size = jnp.minimum(z_index, z_length - z_index).astype(jnp.float32)
    y_size = jnp.minimum(y_index, y_length - y_index).astype(jnp.float32)
    flat = z_size * z_size + y_size * y_size

    def filtered(wave, freq_x):
        size = freq_x.astype(jnp.float32)
        square = flat + size * size
        return split(wave * (square / (square + kerker_wave * kerker_wave)))

    for chunk, (first, end) in enumerate(chunks):
        size = 2 * (end - first)
        base = 2 * first * devices
        land_all(go_copy, chunk)
        for p in range(pencils):
            for f in range(size):
                joined = jnp.concatenate(
                    [
                        land_box[t, pl.ds(base + p * size + f, slabs, stride=pencils * size), :]
                        for t in range(tiles_out)
                    ],
                    axis=1,
                )
                for z in range(z_local):
                    planes[
                        2 * first + f, z * slabs:(z + 1) * slabs, p * y_local:(p + 1) * y_local
                    ] = joined[:, z * y_local:(z + 1) * y_local]
        block = split(planes[2 * first:2 * end].reshape(size * z_length, y_length))
        along_cosine = three(block, y_cosine, ((1,), (0,)))
        along_sine = three(block, y_sine, ((1,), (0,)))
        extra = first == 0
        for k in range(first, end):
            top, low = 2 * (k - first) * z_length, (2 * (k - first) + 1) * z_length
            stop = low + z_length
            real = along_cosine[top:low] + along_sine[low:stop]
            imag = along_cosine[low:stop] - along_sine[top:low]
            wave = three(z_forward, split(jnp.concatenate((real, imag), axis=0)), ((1,), (0,)))
            freq_x = me * slots_k + k
            spectrum[k - first] = three(z_back, filtered(wave, freq_x), ((1,), (0,)))
            if k == 0:
                freq_x = jnp.where(me == 0, x_length // 2, freq_x)
                spectrum[end] = three(z_back, filtered(wave, freq_x), ((1,), (0,)))
        used = end - first + (1 if extra else 0)
        block = split(spectrum[0:used].reshape(used * 2 * z_length, y_length))
        along_cosine = three(block, y_cosine, ((1,), (0,)))
        along_sine = three(block, y_sine, ((1,), (0,)))
        for k in range(first, end):
            top, low = 2 * (k - first) * z_length, (2 * (k - first) + 1) * z_length
            stop = low + z_length
            real = along_cosine[top:low] - along_sine[low:stop]
            if k == 0:
                top, low = 2 * end * z_length, (2 * end + 1) * z_length
                stop = low + z_length
            imag = along_cosine[low:stop] + along_sine[top:low]
            for c, part in enumerate((real, imag)):
                for p in range(pencils):
                    joined = jnp.concatenate(
                        [
                            part[z * slabs:(z + 1) * slabs, p * y_local:(p + 1) * y_local]
                            for z in range(z_local)
                        ],
                        axis=1,
                    )
                    start = base + p * size + 2 * (k - first) + c
                    for t in range(tiles_out):
                        back_box[t, pl.ds(start, slabs, stride=pencils * size), :] = joined[
                            :, t * 128:(t + 1) * 128
                        ]
        start_all(back_copy, chunk)
        field[:, share(chunk, me), :] = back_box[:, share(chunk, me), :]

    for chunk in range(len(chunks)):
        drain_all(go_copy, chunk)
    for chunk in range(len(chunks)):
        land_all(back_copy, chunk)
    for chunk in range(len(chunks)):
        drain_all(back_copy, chunk)


def finish_kernel(field_ref, dens_ref, occ_ref, xb_ref, out_ref, occ_out_ref):
    x_back = (xb_ref[0], xb_ref[1])
    occ_out_ref[...] = occ_ref[...]
    for t in range(field_ref.shape[0]):
        rows = slice(t * 128, (t + 1) * 128)
        out_ref[rows, :] = dens_ref[rows, :] + three(split(field_ref[t]), x_back, ((0,), (0,)))


def fused_body(
    density_history, residual_history, occupancy_history, occupancy_residual, species, slot_count
):
    count, z_local, y_local, x_length = residual_history.shape
    slabs = lax.axis_size("slab")
    pencils = lax.axis_size("pencil")
    devices = slabs * pencils
    z_length, y_length = z_local * slabs, y_local * pencils
    freqs = x_length // devices
    entry = np.arange(ORBITALS * ORBITALS)
    corner = np.maximum(entry // ORBITALS, entry % ORBITALS)[None].astype(np.int32)
    x_forward, x_back, *others = [
        jnp.asarray(t) for t in tables(x_length, y_length, z_length, pencils, slabs)
    ]
    constants = [x_forward, *others]
    chunks = len(cuts_of(freqs // 2))
    vmem = pl.BlockSpec(memory_space=pltpu.VMEM)
    smem = pl.BlockSpec(memory_space=pltpu.SMEM)
    hbm = pl.BlockSpec(memory_space=pltpu.HBM)
    box = (z_local * y_local // 128, devices * freqs, 128)
    sems = pltpu.SemaphoreType.DMA
    flat = jax.ShapeDtypeStruct((z_local * y_local, x_length), jnp.float32)
    blocks = jax.ShapeDtypeStruct(occupancy_history.shape[1:], jnp.float32)
    mixed, mixed_blocks, field = pl.pallas_call(
        functools.partial(
            mix_kernel, slabs, pencils,
            z_length * y_length * x_length, species.shape[0] * devices,
        ),
        out_shape=(flat, blocks, jax.ShapeDtypeStruct(box, jnp.float32)),
        in_specs=[hbm, hbm, vmem, vmem, smem, smem, vmem] + [hbm] * 4,
        out_specs=(vmem, vmem, vmem),
        scratch_shapes=[
            pltpu.VMEM(residual_history.shape, jnp.float32),
            pltpu.VMEM(residual_history.shape, jnp.float32),
            pltpu.VMEM((devices, 1, 128), jnp.float32),
            pltpu.VMEM(box, jnp.float32),
            pltpu.VMEM(box, jnp.float32),
            pltpu.VMEM((freqs, z_length, y_length), jnp.float32),
            pltpu.VMEM((freqs // 2 + 1, 2 * z_length, y_length), jnp.float32),
            pltpu.VMEM(box, jnp.float32),
            *[pltpu.VMEM(t.shape, t.dtype) for t in constants],
            sems((2, z_local)),
            sems((len(constants),)),
            sems((devices,)), sems((devices,)),
            sems((chunks, devices)), sems((chunks, devices)),
            sems((chunks, devices)), sems((chunks, devices)),
        ],
        compiler_params=pltpu.CompilerParams(
            collective_id=0, has_side_effects=True, vmem_limit_bytes=56000 * 1024
        ),
    )(
        residual_history, density_history, occupancy_history, occupancy_residual,
        species, slot_count, jnp.asarray(corner), *constants,
    )
    new_density, new_blocks = pl.pallas_call(
        finish_kernel,
        out_shape=(flat, blocks),
        in_specs=[vmem] * 4,
        out_specs=(vmem, vmem),
    )(field, mixed, mixed_blocks, x_back)
    return new_density.reshape(z_local, y_local, x_length), new_blocks


def solution(mesh):
    placed = (
        P(None, "slab", "pencil", None),
        P(None, "slab", "pencil", None),
        P(None, ("slab", "pencil"), None),
        P(None, ("slab", "pencil"), None),
        P(("slab", "pencil")),
        P(("slab", "pencil")),
    )
    devices = mesh.shape["slab"] * mesh.shape["pencil"]

    def chosen(*arrays):
        x_length = arrays[0].shape[3]
        _, z_local, y_local, _ = arrays[0].shape
        fits = (
            x_length % (2 * devices) == 0
            and mesh.shape["slab"] % 8 == 0
            and y_local % 16 == 0
            and z_local * y_local % 128 == 0
        )
        return (fused_body if fits else body)(*arrays)

    return jax.shard_map(
        chosen,
        mesh=mesh,
        in_specs=placed,
        out_specs=(P("slab", "pencil", None), P(("slab", "pencil"), None)),
        check_vma=False,
    )
```
